32 devices in a mesh: seq: 16 (over z, x, core), chan: 2 (over y).
Axes of the slice: x: 2, y: 2, z: 4, core: 2. Of those that a mesh axis runs over, the one named last changes fastest.
Arguments:
- inner_acts: bfloat16 [8192, 4096], P('seq', 'chan')
- gate_input: bfloat16 [8192, 4096], P('seq', 'chan'), may hold values from -6 to 6
- forward_keys: bfloat16 [8192, 128], P('seq'), may hold values from -0.5 to 0.5
- forward_queries: bfloat16 [8192, 128], P('seq'), may hold values from -6 to 6
- backward_keys: bfloat16 [8192, 128], P('seq'), may hold values from -0.5 to 0.5
- backward_queries: bfloat16 [8192, 128], P('seq'), may hold values from -6 to 6
- decay_codes: int32 [2, 32, 64], P(None, 'seq', 'chan'), may hold values from 1 to 24576
- clip_start: int32 [8192], P('seq'), may hold values 0 or 1
- skip_gain: float32 [64], P('chan'), may hold values from 0.3 to 3
- norm_gain: float32 [4096], P('chan'), may hold values from 0.1 to 1.9
- out_weight: bfloat16 [4096, 2048], P('chan'), may hold values from -0.09375 to 0.09375
Outputs:
- mixed: bfloat16 [2048, 2048], P('seq')
The draws below stay inside these ranges and needn't reach their ends.
All inputs are finite; a program needn't handle non-finite values. No bound on the sum of `clip_start` on one device may be relied on, other than what follows from the above.
Results may differ from the reference program's by a relative error of at most 0.01.
Values may be sent and summed in bfloat16 or wider, within the bound.
No kernel may reach another device: no remote copies, remote signals or barrier semaphores. Data moves between devices by JAX's collectives and lax.ppermute only.
A program may use at most 128 MiB of HBM per device.

```python
import math
import jax
import jax.numpy as jnp
from jax import lax

D = 2048
E = 4096
H = 64
N = 128
SPAN = 256
POOL = 4
TOK_DEV = 512
P_SIZE = 64
TOKENS = 8192
SPANS = 32
N_SEQ = 16


def draw_inner_acts(key, part):
    first, second = jax.random.split(key, 2)
    column = jnp.arange(E, dtype=jnp.float32) / E
    spread = jax.random.uniform(second, (1, E), jnp.float32, 0.5, 2.0)
    col_scale = 10.0 ** (column[None, :] - 0.5) * spread
    values = jax.random.normal(first, (TOKENS, E), jnp.float32) * col_scale
    return values.astype(jnp.bfloat16)


def draw_decay_codes(key, part):
    first, second, third = jax.random.split(jax.random.fold_in(key, 7), 3)
    slow = jax.random.randint(first, (2, 1, H), 0, 2)
    slow_codes = jax.random.randint(second, (2, SPANS, H), 1, 65)
    fast_codes = jax.random.randint(third, (2, SPANS, H), TOKENS, 3 * TOKENS + 1)
    return jnp.where(slow == 1, slow_codes, fast_codes).astype(jnp.int32)


def place_ends(values, own_key, smallest, top_value):
    longest = values.shape.index(max(values.shape))
    spots = []
    for shift in (0, 1):
        where = [jax.random.randint(jax.random.fold_in(own_key, axis), (), 0, length) for axis, length in enumerate(values.shape)]
        where[longest] = (where[longest] + shift) % values.shape[longest]
        spots.append(tuple(where))
    return values.at[spots[0]].set(smallest).at[spots[1]].set(top_value)


def block_scale(rng, shape, shards, low, top_value):
    level = 1.0
    for position, shards_of in shards:
        heights = jax.random.uniform(jax.random.fold_in(jax.random.fold_in(rng, 6), position), (shards_of,), jnp.float32, low / len(shards), top_value / len(shards))
        level = level * jnp.repeat(jnp.exp(heights), shape[position] // shards_of).reshape((-1,) + (1,) * (len(shape) - 1 - position))
    return level


def noise(rng, shape, width, most, shards=(), kind=jnp.bfloat16):
    values = width * jax.random.normal(rng, shape, jnp.float32)
    if shards:
        values = values * block_scale(rng, shape, shards, -0.22, 0.18)
    return jnp.clip(values, -most, most).astype(kind)


def setup_inputs(seed: int = 0) -> dict:
    arg_keys = jax.random.split(jax.random.key(seed), 12)
    inner_acts = draw_inner_acts(jax.random.fold_in(arg_keys[11], 71), 0)
    gate_input = noise(arg_keys[1], (TOKENS, E), 1.0, 6.0, ((0, 16), (1, 2)))
    forward_keys = noise(arg_keys[2], (TOKENS, N), N ** -0.5, 0.5, ((0, 16),))
    forward_queries = noise(arg_keys[3], (TOKENS, N), 1.0, 6.0, ((0, 16),))
    backward_keys = noise(arg_keys[4], (TOKENS, N), N ** -0.5, 0.5, ((0, 16),))
    backward_queries = noise(arg_keys[5], (TOKENS, N), 1.0, 6.0, ((0, 16),))
    decay_codes = draw_decay_codes(jax.random.fold_in(arg_keys[11], 71), 0)
    clip_start = place_ends((jax.random.randint(arg_keys[7], (TOKENS,), 0, TOKENS) < 4).astype(jnp.int32), jax.random.fold_in(arg_keys[7], 1), 0, 1)
    skip_gain = jnp.clip(jnp.exp(math.log(3.0) - 2.3025851 * jax.random.uniform(arg_keys[8], (H,), jnp.float32) ** block_scale(arg_keys[8], (H,), ((0, 2),), -0.2, 0.2)), 0.3, 3.0)
    norm_gain = jnp.clip(1.0 + 0.18 * jax.random.normal(arg_keys[9], (E,), jnp.float32), 0.1, 1.9)
    out_weight = noise(arg_keys[10], (E, D), E ** -0.5, 0.09375, ((0, 2),))
    return dict(inner_acts=inner_acts, gate_input=gate_input, forward_keys=forward_keys, forward_queries=forward_queries, backward_keys=backward_keys, backward_queries=backward_queries, decay_codes=decay_codes, clip_start=clip_start, skip_gain=skip_gain, norm_gain=norm_gain, out_weight=out_weight)


def block_terms(acts, keys, queries, logs, scal, starts, forward):
    seg = jnp.cumsum(starts).astype(jnp.int32)
    cum = jnp.cumsum(logs, axis=0)
    excl = cum - logs
    scores = jnp.dot(queries, keys.T, preferred_element_type=jnp.float32)
    length = keys.shape[0]
    rows_idx = lax.broadcasted_iota(jnp.int32, (length, length), 0)
    cols_idx = lax.broadcasted_iota(jnp.int32, (length, length), 1)
    same = seg[:, None] == seg[None, :]
    cumt = cum.T
    exct = excl.T
    if forward:
        inside = same & (cols_idx <= rows_idx)
        expo = cumt[:, :, None] - cumt[:, None, :]
    else:
        inside = same & (cols_idx >= rows_idx)
        expo = exct[:, None, :] - exct[:, :, None]
    factor = jnp.exp(jnp.where(inside[None], expo, -jnp.inf))
    weights = (factor * scores[None] * scal.T[:, None, :]).astype(jnp.bfloat16)
    final = seg[-1]
    top = cum[-1]
    if forward:
        state_w = jnp.exp(jnp.where((seg == final)[:, None], top[None, :] - cum, -jnp.inf))
        carry_w = jnp.exp(jnp.where((seg == 0)[:, None], cum, -jnp.inf))
    else:
        state_w = jnp.exp(jnp.where((seg == 0)[:, None], excl, -jnp.inf))
        carry_w = jnp.exp(jnp.where((seg == final)[:, None], top[None, :] - excl, -jnp.inf))
    keyed = ((state_w * scal).T[:, :, None] * keys.astype(jnp.float32)[None]).astype(jnp.bfloat16)
    passing = jnp.where(final == 0, jnp.exp(top), jnp.zeros_like(top))
    return (weights, keyed, passing, carry_w)

def direction(acts3, keys, queries, logs, scal, starts, forward):
    items = (acts3.reshape(N_SEQ, TOK_DEV, H, P_SIZE), keys.reshape(N_SEQ, TOK_DEV, N), queries.reshape(N_SEQ, TOK_DEV, N), logs.reshape(N_SEQ, TOK_DEV, H), scal.reshape(N_SEQ, TOK_DEV, H), starts.reshape(N_SEQ, TOK_DEV))

    def step(state, item):
        acts, kb, qb, lg, sc, st = item
        weights, keyed, passing, carry_w = block_terms(acts, kb, qb, lg, sc, st, forward)
        acts_f = acts.astype(jnp.float32)
        inner = jnp.einsum('gij,jgp->igp', weights.astype(jnp.float32), acts_f)
        entering = jnp.einsum('in,gnp->igp', qb.astype(jnp.float32), state, precision=lax.Precision.HIGHEST)
        out_rows = inner + carry_w[:, :, None] * entering
        local = jnp.einsum('gjn,jgp->gnp', keyed.astype(jnp.float32), acts_f)
        return (passing[:, None, None] * state + local, out_rows)
    init = jnp.zeros((H, N, P_SIZE), jnp.float32)
    _, outs = lax.scan(step, init, items, reverse=not forward)
    return outs.reshape(TOKENS, H, P_SIZE)

def reference(inner_acts, gate_input, forward_keys, forward_queries, backward_keys, backward_queries, decay_codes, clip_start, skip_gain, norm_gain, out_weight):
    rate = decay_codes.astype(jnp.float32) / (32.0 * TOKENS)
    rate = jnp.repeat(rate, SPAN, axis=1)
    logs = jnp.log1p(-rate)
    scal = jnp.sqrt(rate * (2.0 - rate))
    acts3 = inner_acts.reshape(TOKENS, H, P_SIZE)
    ahead = direction(acts3, forward_keys, forward_queries, logs[0], scal[0], clip_start, True)
    behind = direction(acts3, backward_keys, backward_queries, logs[1], scal[1], clip_start, False)
    total = ahead + behind + skip_gain[None, :, None] * acts3.astype(jnp.float32)
    gated = total.reshape(TOKENS, E) * jax.nn.silu(gate_input.astype(jnp.float32))
    meansq = lax.optimization_barrier(jnp.sum(gated * gated, axis=1)) / E
    hidden = (gated * lax.rsqrt(meansq + 1e-05)[:, None] * norm_gain[None, :]).astype(jnp.bfloat16)
    projected = jnp.dot(hidden, out_weight, preferred_element_type=jnp.float32)
    mixed = lax.optimization_barrier(jnp.sum(projected.reshape(TOKENS // POOL, POOL, D), axis=1)) * (1.0 / POOL)
    return mixed.astype(jnp.bfloat16)
```

```python
import functools
import math

import jax
import jax.numpy as jnp
from jax import lax
from jax.experimental import pallas as pl
from jax.experimental.pallas import tpu as pltpu
from jax.sharding import PartitionSpec as P

POOL = 4
EPS = 1e-05
LOG2E = math.log2(math.e)
F32 = jnp.float32
BF16 = jnp.bfloat16


def params(priority=None, **kw):
    return pltpu.CompilerParams(dimension_semantics=("arbitrary",), vmem_limit_bytes=56 * 1024 * 1024, **kw)


def dot(a, b, dims=((1,), (0,)), precision=None):
    return lax.dot_general(a, b, (dims, ((), ())), precision=precision, preferred_element_type=F32)


def token_masks(row):
    span = row.shape[1]
    rows = lax.broadcasted_iota(jnp.int32, (span, span), 0)
    cols = lax.broadcasted_iota(jnp.int32, (span, span), 1)
    seg = jnp.sum(jnp.where(cols <= rows, row, 0.0), axis=1, keepdims=True)
    count = jnp.sum(row, axis=1, keepdims=True)
    return seg, count, rows, cols


def local_kernel(core, x, kf, kb, logd, scal, clip, send, keep, midf, midb, xf, xb, pas):
    span = clip.shape[1]
    pos = lax.broadcasted_iota(jnp.int32, (span, 1), 0).astype(F32)
    own_f = core[0] == 1
    lf, lb, pf, pb, df, db = [], [], [], [], [], []
    for s in range(2):
        at = slice(s * span, (s + 1) * span)
        seg, count, _, _ = token_masks(clip[s : s + 1, :].astype(F32))
        key_f = jnp.where(seg == count, kf[at, :].astype(F32), 0.0).astype(BF16)
        key_b = jnp.where(seg == 0.0, kb[at, :].astype(F32), 0.0).astype(BF16)
        acts = x[at, :].astype(F32)
        log_f, log_b = logd[s : s + 1, :], logd[2 + s : 3 + s, :]
        sc_f, sc_b = scal[s : s + 1, :], scal[2 + s : 3 + s, :]
        xs_f = (acts * (sc_f * jnp.exp2((span - 1.0 - pos) * log_f))).astype(BF16)
        xs_b = (acts * (sc_b * jnp.exp2(pos * log_b))).astype(BF16)
        xf[at, :] = xs_f
        xb[at, :] = xs_b
        lf.append(dot(key_f, xs_f, ((0,), (0,))))
        lb.append(dot(key_b, xs_b, ((0,), (0,))))
        whole = count == 0.0
        d_f, d_b = jnp.exp2(span * log_f), jnp.exp2(span * log_b)
        df.append(d_f)
        db.append(d_b)
        pf.append(jnp.where(whole, d_f, 0.0))
        pb.append(jnp.where(whole, d_b, 0.0))
    loc_f = pf[1] * lf[0] + lf[1]
    loc_b = lb[0] + pb[0] * lb[1]
    send[...] = jnp.where(own_f, loc_b, loc_f).astype(BF16)
    keep[...] = jnp.where(own_f, loc_f, loc_b)
    midf[...] = lf[0].astype(BF16)
    midb[...] = lb[1].astype(BF16)
    all_f, all_b = pf[0] * pf[1], pb[0] * pb[1]
    pas[...] = jnp.concatenate(
        [jnp.where(own_f, all_f, all_b), jnp.where(own_f, all_b, all_f), pf[0], pb[1], df[0], df[1], db[0], db[1]], axis=0
    )


def inner_kernel(x, gate, xf, xb, kf, kb, qf, qb, logd, skip, clip, yg, gf, gb, scores):
    span = clip.shape[1]

    @pl.when(pl.program_id(0) == 0)
    def _():
        for s in range(2):
            at = slice(s * span, (s + 1) * span)
            row = clip[s : s + 1, :].astype(F32)
            seg, _, rows, cols = token_masks(row)
            upto = jnp.where(rows <= cols, 1.0, 0.0).astype(BF16)
            seg_row = dot(jnp.broadcast_to(row, (8, span)).astype(BF16), upto)[0:1, :]
            same = seg == seg_row
            sf = dot(qf[at, :], kf[at, :], ((1,), (1,)))
            sb = dot(qb[at, :], kb[at, :], ((1,), (1,)))
            scores[2 * s] = jnp.where(same & (cols <= rows), sf, 0.0).astype(BF16)
            scores[2 * s + 1] = jnp.where(same & (cols >= rows), sb, 0.0).astype(BF16)

    pos = lax.broadcasted_iota(jnp.int32, (span, 1), 0).astype(F32)
    for s in range(2):
        at = slice(s * span, (s + 1) * span)
        out_f = jnp.exp2((pos - (span - 1.0)) * logd[s : s + 1, :])
        out_b = jnp.exp2(-pos * logd[2 + s : 3 + s, :])
        z = gate[at, :].astype(F32)
        g = z / (1.0 + jnp.exp(-z))
        g_f, g_b = g * out_f, g * out_b
        y = g_f * dot(scores[2 * s], xf[at, :]) + g_b * dot(scores[2 * s + 1], xb[at, :])
        yg[at, :] = y + g * (skip[...] * x[at, :].astype(F32))
        gf[at, :] = g_f.astype(BF16)
        gb[at, :] = g_b.astype(BF16)


def carry_kernel(yg, gf, gb, sf, sb, midf, midb, pas, qf, qb, clip, gated, squares, query, acc):
    span = clip.shape[1]

    @pl.when(pl.program_id(0) == 0)
    def _():
        acc[...] = jnp.zeros_like(acc)
        for s in range(2):
            at = slice(s * span, (s + 1) * span)
            seg, count, _, _ = token_masks(clip[s : s + 1, :].astype(F32))
            query[0, at, :] = jnp.where(seg == 0.0, qf[at, :].astype(F32), 0.0).astype(BF16)
            query[1, at, :] = jnp.where(seg == count, qb[at, :].astype(F32), 0.0).astype(BF16)

    p = pas[...]
    st_f, st_b = sf[...].astype(F32), sb[...].astype(F32)
    in_f = [st_f, p[2:3] * st_f + midf[...].astype(F32)]
    in_b = [p[3:4] * st_b + midb[...].astype(F32), st_b]
    for s in range(2):
        at = slice(s * span, (s + 1) * span)
        c_f = dot(query[0, at, :], (p[4 + s : 5 + s] * in_f[s]).astype(BF16))
        c_b = dot(query[1, at, :], (p[6 + s : 7 + s] * in_b[s]).astype(BF16))
        v = yg[at, :] + gf[at, :].astype(F32) * c_f + gb[at, :].astype(F32) * c_b
        gated[at, :] = v.astype(BF16)
        sq = v * v
        lanes = acc.shape[1]
        tot = acc[at, :]
        for k in range(sq.shape[1] // lanes):
            tot = tot + sq[:, k * lanes : (k + 1) * lanes]
        acc[at, :] = tot

    @pl.when(pl.program_id(0) == pl.num_programs(0) - 1)
    def _():
        ones = jnp.ones((8, acc.shape[1]), F32)
        squares[...] = dot(ones, acc[...], ((1,), (1,)), precision=lax.Precision.HIGHEST)


def project_kernel(width, gated, own, other, gain, weight, out, pooled):
    @pl.when(pl.program_id(0) == 0)
    def _():
        rows, tokens = pooled.shape[0], gated.shape[0]
        inv = lax.rsqrt((own[0:1, :] + other[0:1, :]) / width + EPS) * (1.0 / POOL)
        group = lax.broadcasted_iota(jnp.int32, (rows, tokens), 0)
        token = lax.broadcasted_iota(jnp.int32, (rows, tokens), 1)
        pool = jnp.where(token // POOL == group, inv, 0.0)
        high = pool.astype(BF16)
        low = (pool - high.astype(F32)).astype(BF16)
        mixed = dot(high, gated[...]) + dot(low, gated[...])
        pooled[...] = (mixed * gain[...]).astype(BF16)

    out[...] = dot(pooled[...], weight[...]).astype(BF16)


def swap(x, axis, bit):
    size = lax.axis_size(axis)
    return lax.ppermute(x, axis, [(i, i ^ bit) for i in range(size)])


def hop(x, steps):
    size = lax.axis_size("seq")
    pairs = []
    for i in range(size):
        j = i + 4 * steps if i % 2 == 1 else i - 4 * steps
        if 0 <= j < size:
            pairs.append((i, j))
    return lax.ppermute(x, "seq", pairs)


def group_scan(total, keep):
    groups = lax.axis_size("seq") // 4
    if groups <= 4:
        state = jnp.zeros_like(total, F32)
        decays = [hop(keep, k) for k in range(1, groups - 1)]
        parts = [hop(total, k) for k in range(1, groups)]
        for k in range(groups - 1, 0, -1):
            state = parts[k - 1].astype(F32) + (decays[k - 1] * state if k < groups - 1 else 0.0)
        return state
    step = 1
    while step < groups:
        t, d = hop(total, step), hop(keep, step)
        total = (total.astype(F32) + keep * t.astype(F32)).astype(BF16)
        keep = keep * d
        step *= 2
    return hop(total, 1).astype(F32)


def body(
    inner_acts,
    gate_input,
    forward_keys,
    forward_queries,
    backward_keys,
    backward_queries,
    decay_codes,
    clip_start,
    skip_gain,
    norm_gain,
    out_weight,
):
    tokens, channels = inner_acts.shape
    heads = skip_gain.shape[0]
    size = channels // heads
    spans = decay_codes.shape[1]
    span = tokens // spans
    nstate = forward_keys.shape[1]
    model = out_weight.shape[1]
    chan = lax.axis_size("chan")
    width = channels * chan
    index = lax.axis_index("seq")
    core = index % 2
    side = (index // 2) % 2
    half = channels // 2

    codes = jnp.broadcast_to(decay_codes.reshape(2 * spans, heads, 1), (2 * spans, heads, size)).reshape(2 * spans, channels)
    rate = codes.astype(F32) / (32.0 * (lax.axis_size("seq") * tokens))
    logd = jnp.log1p(-rate) * LOG2E
    scal = jnp.sqrt(rate * (2.0 - rate))
    clip = clip_start.reshape(spans, span)
    skip = jnp.broadcast_to(skip_gain[:, None], (heads, size)).reshape(1, channels)
    gain = norm_gain.reshape(1, channels)

    block = min(512, channels)
    steps = channels // block
    tile = lambda rows: pl.BlockSpec((rows, block), lambda i, *_: (0, i))
    full = lambda rows, cols: pl.BlockSpec((rows, cols), lambda i, *_: (0, 0))
    shape = jax.ShapeDtypeStruct

    send, keep, midf, midb, xf, xb, pas = pl.pallas_call(
        local_kernel,
        grid_spec=pltpu.PrefetchScalarGridSpec(
            num_scalar_prefetch=1,
            grid=(steps,),
            in_specs=[
                tile(tokens), full(tokens, nstate), full(tokens, nstate), tile(2 * spans), tile(2 * spans), full(spans, span),
            ],
            out_specs=[tile(nstate), tile(nstate), tile(nstate), tile(nstate), tile(tokens), tile(tokens), tile(8)],
        ),
        out_shape=[
            shape((nstate, channels), BF16), shape((nstate, channels), F32), shape((nstate, channels), BF16),
            shape((nstate, channels), BF16), shape((tokens, channels), BF16), shape((tokens, channels), BF16),
            shape((8, channels), F32),
        ],
        compiler_params=params(),
        name="local",
    )(core.reshape(1).astype(jnp.int32), inner_acts, forward_keys, backward_keys, logd, scal, clip)

    pick = lambda a, b, flag: jnp.where(flag, a, b)
    mine = lambda v: pick(v[:, :half], v[:, half:], side == 0)
    theirs = lambda v: pick(v[:, half:], v[:, :half], side == 0)
    later = side == core

    pass_own, pass_give = pas[0:1], pas[1:2]
    recv1 = swap(send, "seq", 1)
    pass_peer = swap(pass_give, "seq", 1)
    chip = pass_own * recv1.astype(F32) + keep
    chip_pass = pass_own * pass_peer
    recv2 = swap(theirs(chip).astype(BF16), "seq", 2)
    chip_pass_x = swap(chip_pass, "seq", 2)
    chip_h, q_own, q_x = mine(chip), mine(chip_pass), mine(chip_pass_x)
    other_chip = recv2.astype(F32)
    total = pick(q_own * other_chip + chip_h, q_x * chip_h + other_chip, later).astype(BF16)

    yg, gf, gb = pl.pallas_call(
        inner_kernel,
        grid=(steps,),
        in_specs=[
            tile(tokens), tile(tokens), tile(tokens), tile(tokens), full(tokens, nstate), full(tokens, nstate),
            full(tokens, nstate), full(tokens, nstate), tile(2 * spans), tile(1), full(spans, span),
        ],
        out_specs=[tile(tokens), tile(tokens), tile(tokens)],
        out_shape=[shape((tokens, channels), F32), shape((tokens, channels), BF16), shape((tokens, channels), BF16)],
        scratch_shapes=[pltpu.VMEM((2 * spans, span, span), BF16)],
        compiler_params=params(),
        cost_estimate=pl.CostEstimate(flops=4 * 10**9, transcendentals=0, bytes_accessed=16 * 2**20),
        name="inner",
    )(inner_acts, gate_input, xf, xb, forward_keys, backward_keys, forward_queries, backward_queries, logd, skip, clip)

    state = group_scan(total, q_own * q_x)
    recv4 = swap(pick(state, q_own * state + chip_h, later).astype(BF16), "seq", 2)
    entry = pick(q_x * state + other_chip, state, later).astype(BF16)
    chip_state = pick(
        jnp.concatenate([entry, recv4], axis=1), jnp.concatenate([recv4, entry], axis=1), side == 0
    )
    recv5 = swap(chip_state, "seq", 1)
    own_state = (pass_peer * chip_state.astype(F32) + recv1.astype(F32)).astype(BF16)
    state_f = pick(own_state, recv5, core == 1)
    state_b = pick(recv5, own_state, core == 1)

    gated, squares = pl.pallas_call(
        carry_kernel,
        grid=(steps,),
        in_specs=[
            tile(tokens), tile(tokens), tile(tokens), tile(nstate), tile(nstate), tile(nstate), tile(nstate), tile(8),
            full(tokens, nstate), full(tokens, nstate), full(spans, span),
        ],
        out_specs=[tile(tokens), full(8, tokens)],
        out_shape=[shape((tokens, channels), BF16), shape((8, tokens), F32)],
        scratch_shapes=[pltpu.VMEM((2, tokens, nstate), BF16), pltpu.VMEM((tokens, 128), F32)],
        compiler_params=params(),
        name="carry",
    )(yg, gf, gb, state_f, state_b, midf, midb, pas, forward_queries, backward_queries, clip)

    if chan == 2:
        others = swap(squares, "chan", 1)
    else:
        others = lax.psum(squares, "chan") - squares

    cols = min(512, model)
    part = pl.pallas_call(
        functools.partial(project_kernel, float(width)),
        grid=(model // cols,),
        in_specs=[
            full(tokens, channels), full(8, tokens), full(8, tokens), full(1, channels),
            pl.BlockSpec((channels, cols), lambda i: (0, i)),
        ],
        out_specs=pl.BlockSpec((tokens // POOL, cols), lambda i: (0, i)),
        out_shape=shape((tokens // POOL, model), BF16),
        scratch_shapes=[pltpu.VMEM((tokens // POOL, channels), BF16)],
        compiler_params=params(),
        name="project",
    )(gated, squares, others, gain, out_weight)
    if chan == 2:
        peer = swap(part, "chan", 1)
        return (part.astype(F32) + peer.astype(F32)).astype(BF16)
    return lax.psum(part.astype(F32), "chan").astype(BF16)


def solution(mesh):
    placed = (
        P("seq", "chan"),
        P("seq", "chan"),
        P("seq", None),
        P("seq", None),
        P("seq", None),
        P("seq", None),
        P(None, "seq", "chan"),
        P("seq"),
        P("chan"),
        P("chan"),
        P("chan", None),
    )
    return jax.shard_map(body, mesh=mesh, in_specs=placed, out_specs=P("seq", None), check_vma=False)
```

```python
import functools
import math

import jax
import jax.numpy as jnp
from jax import lax
from jax.experimental import pallas as pl
from jax.experimental.pallas import tpu as pltpu
from jax.sharding import PartitionSpec as P

POOL = 4
EPS = 1e-05
LOG2E = math.log2(math.e)
F32 = jnp.float32
BF16 = jnp.bfloat16


VM = pl.BlockSpec(memory_space=pltpu.VMEM)


def params(grid=True, mib=16):
    kw = {"dimension_semantics": ("arbitrary",)} if grid else {}
    return pltpu.CompilerParams(vmem_limit_bytes=mib * 1024 * 1024, **kw)


def vmem(x):
    return pltpu.with_memory_space_constraint(x, pltpu.VMEM)


def hbm(x):
    return pltpu.with_memory_space_constraint(x, pltpu.HBM)


def dot(a, b, dims=((1,), (0,)), precision=None):
    return lax.dot_general(a, b, (dims, ((), ())), precision=precision, preferred_element_type=F32)


def place():
    index = lax.axis_index("seq")
    block = index // 8
    return index % 2 == 1, (index // 2) % 4, block, 2 * (block % 2)


def lanes(start, count):
    return pl.ds(pl.multiple_of(start, 128), count)


def split_rows(v):
    high = v.astype(BF16)
    low = (v - high.astype(F32)).astype(BF16)
    return jnp.concatenate([high, low, jnp.zeros((6, v.shape[1]), BF16)], axis=0)


def joined(ref, nstate, at=slice(None)):
    rows = ref[nstate : nstate + 8, at].astype(F32)
    return rows[0:1] + rows[1:2]


def token_masks(row):
    span = row.shape[1]
    rows = lax.broadcasted_iota(jnp.int32, (span, span), 0)
    cols = lax.broadcasted_iota(jnp.int32, (span, span), 1)
    seg = jnp.sum(jnp.where(cols <= rows, row, 0.0), axis=1, keepdims=True)
    count = jnp.sum(row, axis=1, keepdims=True)
    return seg, count, rows, cols


def local_kernel(total, size, x, kf, kb, codes, skip, clip, send, keep, midf, midb, rows, keys):
    spans = 2
    span = clip.shape[1] // spans
    block = x.shape[1]
    nstate = kf.shape[1]
    step = pl.program_id(0)
    own_f, _, _, _ = place()
    wholes = []
    for s in range(spans):
        at = slice(s * span, (s + 1) * span)
        row = clip[0:1, at].astype(F32)
        wholes.append(jnp.sum(row, axis=1, keepdims=True) == 0.0)

    @pl.when(step == 0)
    def _():
        for s in range(spans):
            at = slice(s * span, (s + 1) * span)
            seg, count, _, _ = token_masks(clip[0:1, at].astype(F32))
            keys[0, at, :] = jnp.where(seg == count, kf[at, :].astype(F32), 0.0).astype(BF16)
            keys[1, at, :] = jnp.where(seg == 0.0, kb[at, :].astype(F32), 0.0).astype(BF16)

    heads = codes.shape[1]
    table = jnp.concatenate([codes[...].astype(F32), skip[...], jnp.zeros((3, heads), F32)], axis=0)
    lane = lax.broadcasted_iota(jnp.int32, (heads, block), 1) + step * block
    pick = lax.broadcasted_iota(jnp.int32, (heads, block), 0) == lane // size
    wide = dot(table, jnp.where(pick, 1.0, 0.0), precision=lax.Precision.HIGHEST)
    rate = wide[0:4] * (1.0 / (32.0 * total))
    logd = jnp.log1p(-rate) * LOG2E
    scal = jnp.sqrt(rate * (2.0 - rate))

    pos = lax.broadcasted_iota(jnp.int32, (span, 1), 0).astype(F32)
    lf, lb, pf, pb, df, db = [], [], [], [], [], []
    for s in range(spans):
        at = slice(s * span, (s + 1) * span)
        acts = x[at, :].astype(F32)
        log_f, log_b = logd[s : s + 1], logd[2 + s : 3 + s]
        xs_f = (acts * (scal[s : s + 1] * jnp.exp2((span - 1.0 - pos) * log_f))).astype(BF16)
        xs_b = (acts * (scal[2 + s : 3 + s] * jnp.exp2(pos * log_b))).astype(BF16)
        lf.append(dot(keys[0, at, :], xs_f, ((0,), (0,))))
        lb.append(dot(keys[1, at, :], xs_b, ((0,), (0,))))
        d_f, d_b = jnp.exp2(span * log_f), jnp.exp2(span * log_b)
        df.append(d_f)
        db.append(d_b)
        pf.append(jnp.where(wholes[s], d_f, 0.0))
        pb.append(jnp.where(wholes[s], d_b, 0.0))
    loc_f = pf[1] * lf[0] + lf[1]
    loc_b = lb[0] + pb[0] * lb[1]
    here = lanes(step * block, block)
    all_f, all_b = pf[0] * pf[1], pb[0] * pb[1]
    send[0:nstate, here] = jnp.where(own_f, loc_b, loc_f).astype(BF16)
    send[nstate : nstate + 8, here] = split_rows(jnp.where(own_f, all_b, all_f))
    keep[:, here] = jnp.where(own_f, loc_f, loc_b)
    midf[:, here] = lf[0].astype(BF16)
    midb[:, here] = lb[1].astype(BF16)
    own = jnp.where(own_f, all_f, all_b)
    rows[0:8, here] = jnp.concatenate([own, own, pf[0], pb[1], df[0], df[1], db[0], db[1]], axis=0)
    rows[8:16, here] = jnp.concatenate([logd, scal], axis=0)
    rows[16:24, here] = jnp.concatenate([wide[4:5], wide[1:8]], axis=0)


def inner_kernel(after, x, gate, kf, kb, qf, qb, rows_in, clip, weight, yg, gf, gb, weight_out, scores, sem):
    spans = 2
    span = clip.shape[1] // spans
    block = x.shape[1]
    step = pl.program_id(0)
    fetch = pltpu.make_async_copy(weight, weight_out, sem)

    @pl.when(step == 0)
    def _():
        fetch.start()
        for s in range(spans):
            at = slice(s * span, (s + 1) * span)
            row = clip[0:1, at].astype(F32)
            seg, _, rows, cols = token_masks(row)
            upto = jnp.where(rows <= cols, 1.0, 0.0).astype(BF16)
            seg_row = dot(jnp.broadcast_to(row, (8, span)).astype(BF16), upto)[0:1, :]
            same = seg == seg_row
            sf = dot(qf[at, :], kf[at, :], ((1,), (1,)))
            sb = dot(qb[at, :], kb[at, :], ((1,), (1,)))
            scores[2 * s] = jnp.where(same & (cols <= rows), sf, 0.0).astype(BF16)
            scores[2 * s + 1] = jnp.where(same & (cols >= rows), sb, 0.0).astype(BF16)

    here = lanes(step * block, block)
    logd, scal = rows_in[8:12, here], rows_in[12:16, here]
    skip = rows_in[16:24, here][0:1]
    pos = lax.broadcasted_iota(jnp.int32, (span, 1), 0).astype(F32)
    for s in range(spans):
        at = slice(s * span, (s + 1) * span)
        log_f, log_b = logd[s : s + 1], logd[2 + s : 3 + s]
        acts = x[at, :].astype(F32)
        xs_f = (acts * (scal[s : s + 1] * jnp.exp2((span - 1.0 - pos) * log_f))).astype(BF16)
        xs_b = (acts * (scal[2 + s : 3 + s] * jnp.exp2(pos * log_b))).astype(BF16)
        z = gate[at, :].astype(F32)
        g = z / (1.0 + jnp.exp(-z))
        g_f = g * jnp.exp2((pos - (span - 1.0)) * log_f)
        g_b = g * jnp.exp2(-pos * log_b)
        y = g_f * dot(scores[2 * s], xs_f) + g_b * dot(scores[2 * s + 1], xs_b)
        yg[at, here] = y + g * (skip * acts)
        gf[at, here] = g_f.astype(BF16)
        gb[at, here] = g_b.astype(BF16)

    @pl.when(step == pl.num_programs(0) - 1)
    def _():
        fetch.wait()


def chip_kernel(recv, keep, rows, mine, passes, *sends):
    nstate, part = mine.shape
    _, chip, _, flip = place()
    for k in range(4):
        at = lanes((chip ^ k ^ flip) * part, part)
        own = rows[0:8, at][0:1]
        state = own * recv[0:nstate, at].astype(F32) + keep[:, at]
        both = own * joined(recv, nstate, at)
        if k == 0:
            mine[...] = state
            passes[...] = jnp.broadcast_to(both, (8, part))
        else:
            sends[k - 1][0:nstate, :] = state.astype(BF16)
            sends[k - 1][nstate : nstate + 8, :] = split_rows(both)


def group_kernel(recv_a, recv_b, recv_c, mine, passes, _, total, states, decays):
    nstate = mine.shape[0]
    own_f, chip, _, _ = place()
    states[chip] = mine[...]
    decays[chip] = passes[...]
    for k, recv in enumerate((recv_a, recv_b, recv_c)):
        states[chip ^ (k + 1)] = recv[0:nstate, :].astype(F32)
        decays[chip ^ (k + 1)] = jnp.broadcast_to(joined(recv, nstate), passes.shape)
    first = jnp.where(own_f, 0, 3)
    state, keep = states[first], decays[first][0:1]
    for t in range(1, 4):
        j = jnp.where(own_f, t, 3 - t)
        d = decays[j][0:1]
        state = d * state + states[j]
        keep = keep * d
    total[0:nstate, :] = state.astype(BF16)
    total[nstate : nstate + 8, :] = split_rows(keep)


def join_kernel(mine, recv, total):
    nstate = mine.shape[0] - 8
    keep = joined(mine, nstate)
    total[0:nstate, :] = (mine[0:nstate, :].astype(F32) + keep * recv[0:nstate, :].astype(F32)).astype(BF16)
    total[nstate : nstate + 8, :] = split_rows(keep * joined(recv, nstate))


def entry_kernel(pair, recv, states, decays, entry, send_a, send_b, send_c, ahead):
    nstate = entry.shape[0]
    own_f, chip, block, _ = place()
    state = recv[0:nstate, :].astype(F32)
    if pair:
        state = jnp.where(own_f == (block == 1), state, 0.0)
    for t in range(4):
        j = jnp.where(own_f, t, 3 - t)
        ahead[j] = state
        if t < 3:
            state = decays[j][0:1] * state + states[j]
    for k, out in enumerate((entry, send_a, send_b, send_c)):
        out[...] = ahead[chip ^ k].astype(BF16)


def carry_kernel(block, *refs):
    owns, oths = refs[0:4], refs[4:8]
    yg, gf, gb, recv, midf, midb, rows, qf, qb, clip, gated, squares, query, acc = refs[8:]
    spans = 2
    span = clip.shape[1] // spans
    nstate, part = owns[0].shape
    own_f, chip, _, flip = place()
    acc[...] = jnp.zeros_like(acc)
    for s in range(spans):
        at = slice(s * span, (s + 1) * span)
        seg, count, _, _ = token_masks(clip[0:1, at].astype(F32))
        query[0, at, :] = jnp.where(seg == 0.0, qf[at, :].astype(F32), 0.0).astype(BF16)
        query[1, at, :] = jnp.where(seg == count, qb[at, :].astype(F32), 0.0).astype(BF16)

    width = acc.shape[1]
    for piece in range(4):
        own_ref, oth_ref = owns[piece], oths[piece]
        for j in range(part // block):
            cut = slice(j * block, (j + 1) * block)
            here = lanes((chip ^ piece ^ flip) * part + j * block, block)
            peer = joined(recv, nstate, here)
            own = peer * own_ref[:, cut].astype(F32) + recv[0:nstate, here].astype(F32)
            oth = oth_ref[:, cut].astype(F32)
            st_f, st_b = jnp.where(own_f, own, oth), jnp.where(own_f, oth, own)
            p = rows[0:8, here]
            in_f = [st_f, p[2:3] * st_f + midf[:, here].astype(F32)]
            in_b = [p[3:4] * st_b + midb[:, here].astype(F32), st_b]
            for s in range(spans):
                at = slice(s * span, (s + 1) * span)
                c_f = dot(query[0, at, :], (p[4 + s : 5 + s] * in_f[s]).astype(BF16))
                c_b = dot(query[1, at, :], (p[6 + s : 7 + s] * in_b[s]).astype(BF16))
                v = yg[at, here] + gf[at, here].astype(F32) * c_f + gb[at, here].astype(F32) * c_b
                gated[at, here] = v.astype(BF16)
                sq = v * v
                tot = acc[at, :]
                for k in range(block // width):
                    tot = tot + sq[:, k * width : (k + 1) * width]
                acc[at, :] = tot
    ones = jnp.ones((8, width), F32)
    squares[...] = dot(ones, acc[...], ((1,), (1,)), precision=lax.Precision.HIGHEST)


def project_kernel(width, gated, own, other, gain, weight, out):
    rows, tokens = out.shape[0], gated.shape[0]
    inv = lax.rsqrt((own[0:1, :] + other[0:1, :]) / width + EPS) * (1.0 / POOL)
    group = lax.broadcasted_iota(jnp.int32, (rows, tokens), 0)
    token = lax.broadcasted_iota(jnp.int32, (rows, tokens), 1)
    pool = jnp.where(token // POOL == group, inv, 0.0)
    high = pool.astype(BF16)
    low = (pool - high.astype(F32)).astype(BF16)
    mixed = dot(high, gated[...]) + dot(low, gated[...])
    pooled = (mixed * gain[...]).astype(BF16)
    out[...] = dot(pooled, weight[...]).astype(BF16)


def swap(x, axis, bit):
    size = lax.axis_size(axis)
    return lax.ppermute(x, axis, [(i, i ^ bit) for i in range(size)])


def hop(x, steps):
    size = lax.axis_size("seq")
    pairs = []
    for i in range(size):
        j = (i + 8 * steps if i % 2 == 1 else i - 8 * steps) ^ (4 * (steps % 2))
        if 0 <= j < size:
            pairs.append((i, j))
    return lax.ppermute(x, "seq", pairs)


def call(kernel, outs, *ins, scratch=(), name=None):
    return pl.pallas_call(
        kernel,
        in_specs=[VM] * len(ins),
        out_specs=[VM] * len(outs),
        out_shape=[pltpu.VMEM(*o) for o in outs],
        scratch_shapes=list(scratch),
        compiler_params=params(False),
        name=name,
    )(*[vmem(x) for x in ins])


def body(
    inner_acts,
    gate_input,
    forward_keys,
    forward_queries,
    backward_keys,
    backward_queries,
    decay_codes,
    clip_start,
    skip_gain,
    norm_gain,
    out_weight,
):
    tokens, channels = inner_acts.shape
    heads = skip_gain.shape[0]
    spans = decay_codes.shape[1]
    span = tokens // spans
    nstate = forward_keys.shape[1]
    model = out_weight.shape[1]
    chan = lax.axis_size("chan")
    part = channels // 4
    assert spans == 2

    codes = decay_codes.reshape(2 * spans, heads)
    clip = clip_start.reshape(1, tokens)
    skip = skip_gain.reshape(1, heads)
    gain = norm_gain.reshape(1, channels)

    block = min(512, channels)
    steps = channels // block
    tile = lambda rows: pl.BlockSpec((rows, block), lambda i: (0, i))
    full = lambda x: pl.BlockSpec(x.shape, lambda i: (0, 0))
    vshape = pltpu.VMEM

    send, keep, midf, midb, rows = pl.pallas_call(
        functools.partial(local_kernel, float(lax.axis_size("seq") * tokens), channels // heads),
        grid=(steps,),
        in_specs=[tile(tokens), full(forward_keys), full(backward_keys), full(codes), full(skip), full(clip)],
        out_specs=[VM] * 5,
        out_shape=[
            vshape((nstate + 8, channels), BF16), vshape((nstate, channels), F32), vshape((nstate, channels), BF16),
            vshape((nstate, channels), BF16), vshape((24, channels), F32),
        ],
        scratch_shapes=[pltpu.VMEM((2, tokens, nstate), BF16)],
        compiler_params=params(),
        name="local",
    )(*[hbm(x) for x in (inner_acts, forward_keys, backward_keys, codes, skip, clip)])

    recv1 = swap(send, "seq", 1)
    packed = ((nstate + 8, part), BF16)
    mine, passes, *sends = call(
        chip_kernel, [((nstate, part), F32), ((8, part), F32)] + [packed] * 3, recv1, keep, rows, name="chip"
    )
    recv2 = [swap(x, "seq", 2 * k + 2) for k, x in enumerate(sends)]
    after = sends[0]

    yg, gf, gb, weight = pl.pallas_call(
        inner_kernel,
        grid=(steps,),
        in_specs=[
            VM, tile(tokens), tile(tokens), full(forward_keys), full(forward_keys), full(forward_keys), full(forward_keys),
            VM, full(clip), pl.BlockSpec(memory_space=pltpu.HBM),
        ],
        out_specs=[VM] * 4,
        out_shape=[
            vshape((tokens, channels), F32), vshape((tokens, channels), BF16), vshape((tokens, channels), BF16),
            vshape(out_weight.shape, BF16),
        ],
        scratch_shapes=[pltpu.VMEM((2 * spans, span, span), BF16), pltpu.SemaphoreType.DMA],
        compiler_params=params(),
        cost_estimate=pl.CostEstimate(flops=4 * 10**9, transcendentals=0, bytes_accessed=16 * 2**20),
        name="inner",
    )(
        vmem(after), inner_acts, gate_input, forward_keys, backward_keys, forward_queries, backward_queries, vmem(rows), clip,
        hbm(out_weight),
    )

    total, states, decays = call(
        group_kernel, [packed, ((4, nstate, part), F32), ((4, 8, part), F32)], *recv2, mine, passes, gb, name="group"
    )
    blocks = lax.axis_size("seq") // 8
    if blocks == 2:
        before = swap(total, "seq", 12)
    else:
        step = 1
        while step < blocks:
            (total,) = call(join_kernel, [packed], total, hop(total, step), name="join")
            step *= 2
        before = hop(total, 1)
    own = call(
        functools.partial(entry_kernel, blocks == 2), [((nstate, part), BF16)] * 4, before, states, decays,
        scratch=[pltpu.VMEM((4, nstate, part), F32)], name="entry",
    )
    own = [own[0]] + [swap(x, "seq", 2 * k + 2) for k, x in enumerate(own[1:])]
    peer = [swap(x, "seq", 1) for x in own]
    gated, squares = call(
        functools.partial(carry_kernel, min(block, part)), [((tokens, channels), BF16), ((8, tokens), F32)],
        *own, *peer, yg, gf, gb, recv1, midf, midb, rows, forward_queries, backward_queries, clip,
        scratch=[pltpu.VMEM((2, tokens, nstate), BF16), pltpu.VMEM((tokens, 128), F32)], name="carry",
    )

    if chan == 2:
        own, others = squares, swap(squares, "chan", 1)
    else:
        own = lax.psum(squares, "chan")
        others = jnp.zeros_like(own)
    (mixed,) = call(
        functools.partial(project_kernel, float(channels * chan)), [((tokens // POOL, model), BF16)],
        gated, own, others, gain, weight, name="project",
    )
    if chan == 2:
        peer = swap(mixed, "chan", 1)
        return (mixed.astype(F32) + peer.astype(F32)).astype(BF16)
    return lax.psum(mixed.astype(F32), "chan").astype(BF16)


def solution(mesh):
    placed = (
        P("seq", "chan"),
        P("seq", "chan"),
        P("seq", None),
        P("seq", None),
        P("seq", None),
        P("seq", None),
        P(None, "seq", "chan"),
        P("seq"),
        P("chan"),
        P("chan"),
        P("chan", None),
    )
    return jax.shard_map(body, mesh=mesh, in_specs=placed, out_specs=P("seq", None), check_vma=False)
```

```python
import functools
import math

import jax
import jax.numpy as jnp
from jax import lax
from jax.experimental import pallas as pl
from jax.experimental.pallas import tpu as pltpu
from jax.sharding import PartitionSpec as P


POOL = 4
EPS = 1e-05
LOG2E = math.log2(math.e)
F32 = jnp.float32
BF16 = jnp.bfloat16


VM = pl.BlockSpec(memory_space=pltpu.VMEM)


def params(grid=True, mib=16):
    kw = {"dimension_semantics": ("arbitrary",)} if grid else {}
    return pltpu.CompilerParams(vmem_limit_bytes=mib * 1024 * 1024, **kw)


def vmem(x):
    return pltpu.with_memory_space_constraint(x, pltpu.VMEM)


def hbm(x):
    return pltpu.with_memory_space_constraint(x, pltpu.HBM)


def dot(a, b, dims=((1,), (0,)), precision=None):
    return lax.dot_general(a, b, (dims, ((), ())), precision=precision, preferred_element_type=F32)


def place():
    index = lax.axis_index("seq")
    block = index // 8
    return index % 2 == 1, (index // 2) % 4, block, 2 * (block % 2)


def lanes(start, count):
    return pl.ds(pl.multiple_of(start, 128), count)


def split_rows(v):
    high = v.astype(BF16)
    low = (v - high.astype(F32)).astype(BF16)
    return jnp.concatenate([high, low, jnp.zeros((6, v.shape[1]), BF16)], axis=0)


def joined(ref, nstate, at=slice(None)):
    rows = ref[nstate : nstate + 8, at].astype(F32)
    return rows[0:1] + rows[1:2]


def token_masks(row):
    span = row.shape[1]
    rows = lax.broadcasted_iota(jnp.int32, (span, span), 0)
    cols = lax.broadcasted_iota(jnp.int32, (span, span), 1)
    seg = jnp.sum(jnp.where(cols <= rows, row, 0.0), axis=1, keepdims=True)
    count = jnp.sum(row, axis=1, keepdims=True)
    return seg, count, rows, cols


def local_kernel(total, size, x, kf, kb, codes, skip, clip, send, keep, midf, midb, rows, keys):
    spans = 2
    span = clip.shape[1] // spans
    block = x.shape[1]
    nstate = kf.shape[1]
    step = pl.program_id(0)
    own_f, _, _, _ = place()
    wholes = []
    for s in range(spans):
        at = slice(s * span, (s + 1) * span)
        row = clip[0:1, at].astype(F32)
        wholes.append(jnp.sum(row, axis=1, keepdims=True) == 0.0)

    @pl.when(step == 0)
    def _():
        for s in range(spans):
            at = slice(s * span, (s + 1) * span)
            seg, count, _, _ = token_masks(clip[0:1, at].astype(F32))
            keys[0, at, :] = jnp.where(seg == count, kf[at, :].astype(F32), 0.0).astype(BF16)
            keys[1, at, :] = jnp.where(seg == 0.0, kb[at, :].astype(F32), 0.0).astype(BF16)

    heads = codes.shape[1]
    table = jnp.concatenate([codes[...].astype(F32), skip[...], jnp.zeros((3, heads), F32)], axis=0)
    lane = lax.broadcasted_iota(jnp.int32, (heads, block), 1) + step * block
    pick = lax.broadcasted_iota(jnp.int32, (heads, block), 0) == lane // size
    wide = dot(table, jnp.where(pick, 1.0, 0.0), precision=lax.Precision.HIGHEST)
    rate = wide[0:4] * (1.0 / (32.0 * total))
    logd = jnp.log1p(-rate) * LOG2E
    scal = jnp.sqrt(rate * (2.0 - rate))

    pos = lax.broadcasted_iota(jnp.int32, (span, 1), 0).astype(F32)
    lf, lb, pf, pb, df, db = [], [], [], [], [], []
    for s in range(spans):
        at = slice(s * span, (s + 1) * span)
        acts = x[at, :].astype(F32)
        log_f, log_b = logd[s : s + 1], logd[2 + s : 3 + s]
        xs_f = (acts * (scal[s : s + 1] * jnp.exp2((span - 1.0 - pos) * log_f))).astype(BF16)
        xs_b = (acts * (scal[2 + s : 3 + s] * jnp.exp2(pos * log_b))).astype(BF16)
        lf.append(dot(keys[0, at, :], xs_f, ((0,), (0,))))
        lb.append(dot(keys[1, at, :], xs_b, ((0,), (0,))))
        d_f, d_b = jnp.exp2(span * log_f), jnp.exp2(span * log_b)
        df.append(d_f)
        db.append(d_b)
        pf.append(jnp.where(wholes[s], d_f, 0.0))
        pb.append(jnp.where(wholes[s], d_b, 0.0))
    loc_f = pf[1] * lf[0] + lf[1]
    loc_b = lb[0] + pb[0] * lb[1]
    here = lanes(step * block, block)
    all_f, all_b = pf[0] * pf[1], pb[0] * pb[1]
    send[0:nstate, here] = jnp.where(own_f, loc_b, loc_f).astype(BF16)
    send[nstate : nstate + 8, here] = split_rows(jnp.where(own_f, all_b, all_f))
    keep[:, here] = jnp.where(own_f, loc_f, loc_b)
    midf[:, here] = lf[0].astype(BF16)
    midb[:, here] = lb[1].astype(BF16)
    own = jnp.where(own_f, all_f, all_b)
    rows[0:8, here] = jnp.concatenate([own, own, pf[0], pb[1], df[0], df[1], db[0], db[1]], axis=0)
    rows[8:16, here] = jnp.concatenate([logd, scal], axis=0)
    rows[16:24, here] = jnp.concatenate([wide[4:5], wide[1:8]], axis=0)


def score_kernel(after, kf, kb, qf, qb, clip, scores, query):
    spans = 2
    span = clip.shape[1] // spans
    for s in range(spans):
        at = slice(s * span, (s + 1) * span)
        row = clip[0:1, at].astype(F32)
        seg, count, rows, cols = token_masks(row)
        upto = jnp.where(rows <= cols, 1.0, 0.0).astype(BF16)
        seg_row = dot(jnp.broadcast_to(row, (8, span)).astype(BF16), upto)[0:1, :]
        same = seg == seg_row
        sf = dot(qf[at, :], kf[at, :], ((1,), (1,)))
        sb = dot(qb[at, :], kb[at, :], ((1,), (1,)))
        scores[2 * s] = jnp.where(same & (cols <= rows), sf, 0.0).astype(BF16)
        scores[2 * s + 1] = jnp.where(same & (cols >= rows), sb, 0.0).astype(BF16)
        query[0, at, :] = jnp.where(seg == 0.0, qf[at, :].astype(F32), 0.0).astype(BF16)
        query[1, at, :] = jnp.where(seg == count, qb[at, :].astype(F32), 0.0).astype(BF16)


def inner_kernel(first, *refs):
    after, x, gate, rows, midf, midb, scores, query, weight, *refs = refs
    if first:
        yg, gf, gb, weight_out, sem = refs
    else:
        yg, gf, gb, weight_out, sem = refs[4:]
    spans = 2
    block = x.shape[1]
    span = scores.shape[1]
    step = pl.program_id(0)
    steps = pl.num_programs(0)
    height = weight.shape[0] // 2
    band = pl.ds(0 if first else height, height)
    fetch = pltpu.make_async_copy(weight.at[band], weight_out.at[band], sem)

    @pl.when(step == 0)
    def _():
        fetch.start()

    here = lanes((step + (0 if first else steps)) * block, block)
    p = rows[0:8, here]
    logd, scal = rows[8:12, here], rows[12:16, here]
    skip = rows[16:24, here][0:1]
    pos = lax.broadcasted_iota(jnp.int32, (span, 1), 0).astype(F32)
    for s in range(spans):
        at = slice(s * span, (s + 1) * span)
        log_f, log_b = logd[s : s + 1], logd[2 + s : 3 + s]
        d_f, d_b = p[4 + s : 5 + s], p[6 + s : 7 + s]
        acts = x[at, :].astype(F32)
        xs_f = (acts * (scal[s : s + 1] * jnp.exp2((span - 1.0 - pos) * log_f))).astype(BF16)
        xs_b = (acts * (scal[2 + s : 3 + s] * jnp.exp2(pos * log_b))).astype(BF16)
        z = gate[at, :].astype(F32)
        g = z / (1.0 + jnp.exp(-z))
        g_f = g * jnp.exp2((pos - (span - 1.0)) * log_f)
        g_b = g * jnp.exp2(-pos * log_b)
        y_f, y_b = dot(scores[2 * s], xs_f), dot(scores[2 * s + 1], xs_b)
        if s == 1:
            y_f = y_f + dot(query[0, at, :], (d_f * midf[:, here].astype(F32)).astype(BF16))
            d_f = d_f * p[2:3]
        else:
            y_b = y_b + dot(query[1, at, :], (d_b * midb[:, here].astype(F32)).astype(BF16))
            d_b = d_b * p[3:4]
        yg[at, here] = g_f * y_f + g_b * y_b + g * (skip * acts)
        gf[at, here] = (g_f * d_f).astype(BF16)
        gb[at, here] = (g_b * d_b).astype(BF16)

    @pl.when(step == steps - 1)
    def _():
        fetch.wait()


def chip_kernel(recv, keep, rows, mine, passes, *sends):
    nstate, part = mine.shape
    _, chip, _, flip = place()
    for k in range(4):
        at = lanes((chip ^ k ^ flip) * part, part)
        own = rows[0:8, at][0:1]
        state = own * recv[0:nstate, at].astype(F32) + keep[:, at]
        both = own * joined(recv, nstate, at)
        if k == 0:
            mine[...] = state
            passes[...] = jnp.broadcast_to(both, (8, part))
        else:
            sends[k - 1][0:nstate, :] = state.astype(BF16)
            sends[k - 1][nstate : nstate + 8, :] = split_rows(both)


def group_kernel(recv_a, recv_b, recv_c, mine, passes, _, total, states, decays):
    nstate = mine.shape[0]
    own_f, chip, _, _ = place()
    states[chip] = mine[...]
    decays[chip] = passes[...]
    for k, recv in enumerate((recv_a, recv_b, recv_c)):
        states[chip ^ (k + 1)] = recv[0:nstate, :].astype(F32)
        decays[chip ^ (k + 1)] = jnp.broadcast_to(joined(recv, nstate), passes.shape)
    first = jnp.where(own_f, 0, 3)
    state, keep = states[first], decays[first][0:1]
    for t in range(1, 4):
        j = jnp.where(own_f, t, 3 - t)
        d = decays[j][0:1]
        state = d * state + states[j]
        keep = keep * d
    total[0:nstate, :] = state.astype(BF16)
    total[nstate : nstate + 8, :] = split_rows(keep)


def join_kernel(mine, recv, total):
    nstate = mine.shape[0] - 8
    keep = joined(mine, nstate)
    total[0:nstate, :] = (mine[0:nstate, :].astype(F32) + keep * recv[0:nstate, :].astype(F32)).astype(BF16)
    total[nstate : nstate + 8, :] = split_rows(keep * joined(recv, nstate))


def entry_kernel(pair, recv, states, decays, _, entry, send_a, send_b, send_c, ahead):
    nstate = entry.shape[0]
    own_f, chip, block, _ = place()
    state = recv[0:nstate, :].astype(F32)
    if pair:
        state = jnp.where(own_f == (block == 1), state, 0.0)
    for t in range(4):
        j = jnp.where(own_f, t, 3 - t)
        ahead[j] = state
        if t < 3:
            state = decays[j][0:1] * state + states[j]
    for k, out in enumerate((entry, send_a, send_b, send_c)):
        out[...] = ahead[chip ^ k].astype(BF16)


def carry_kernel(pieces, tokens, last, *refs):
    count = len(pieces)
    own_refs, oth_refs, refs = refs[:count], refs[count : 2 * count], refs[2 * count :]
    yg, gf, gb, recv, query, gain, *refs = refs
    before = None if pieces[0] == 0 else refs.pop(0)
    gated, sums = refs[:count], refs[count]
    own_f, chip, _, flip = place()
    nstate, part = own_refs[0].shape
    at = slice(*tokens)
    rel = slice(0, tokens[1] - tokens[0])
    acc = jnp.zeros((tokens[1] - tokens[0], 128), F32) if before is None else before[at, :]
    for own_ref, oth_ref, out, piece in zip(own_refs, oth_refs, gated, pieces):
        here = lanes((chip ^ piece ^ flip) * part, part)
        own = joined(recv, nstate, here) * own_ref[...].astype(F32) + recv[0:nstate, here].astype(F32)
        oth = oth_ref[...].astype(F32)
        st_f, st_b = jnp.where(own_f, own, oth).astype(BF16), jnp.where(own_f, oth, own).astype(BF16)
        c_f = dot(query[0, at, :], st_f)
        c_b = dot(query[1, at, :], st_b)
        v = yg[at, here] + gf[at, here].astype(F32) * c_f + gb[at, here].astype(F32) * c_b
        out[rel, :] = (v * gain[0:1, here]).astype(BF16)
        sq = v * v
        for k in range(part // 128):
            acc = acc + sq[:, k * 128 : (k + 1) * 128]
    if last:
        ones = jnp.ones((8, 128), BF16)
        high = acc.astype(BF16)
        low = (acc - high.astype(F32)).astype(BF16)
        sums[...] = dot(ones, high, ((1,), (1,))) + dot(ones, low, ((1,), (1,)))
    else:
        sums[...] = acc


def early_kernel(pieces_a, pieces_b, pieces_c, pieces_d, weight, high, low):
    part = pieces_a.shape[1]
    _, chip, _, flip = place()
    total = None
    for k, ref in enumerate((pieces_a, pieces_b, pieces_c, pieces_d)):
        at = lanes((chip ^ k ^ flip) * part, part)
        term = dot(ref[...], weight[at, 0 : high.shape[1]])
        total = term if total is None else total + term
    high[...] = total.astype(BF16)
    low[...] = (total - high[...].astype(F32)).astype(BF16)


def first_kernel(width, own, other, tokens_high, tokens_low, out, pool_high, pool_low):
    rows, tokens = pool_high.shape
    inv = lax.rsqrt((own[0:1, :] + other[0:1, :]) / width + EPS) * (1.0 / POOL)
    group = lax.broadcasted_iota(jnp.int32, (rows, tokens), 0)
    token = lax.broadcasted_iota(jnp.int32, (rows, tokens), 1)
    pool = jnp.where(token // POOL == group, inv, 0.0)
    high = pool.astype(BF16)
    low = (pool - high.astype(F32)).astype(BF16)
    pool_high[...] = high
    pool_low[...] = low
    out[...] = (dot(high, tokens_high[...]) + dot(high, tokens_low[...]) + dot(low, tokens_high[...])).astype(BF16)


def pool_kernel(pieces_a, pieces_b, pieces_c, pieces_d, high, low, pooled):
    part = pieces_a.shape[1]
    _, chip, _, flip = place()
    for k, ref in enumerate((pieces_a, pieces_b, pieces_c, pieces_d)):
        at = lanes((chip ^ k ^ flip) * part, part)
        pooled[:, at] = (dot(high[...], ref[...]) + dot(low[...], ref[...])).astype(BF16)


def project_kernel(start, pooled, weight, out):
    out[...] = dot(pooled[...], weight[:, start : start + out.shape[1]]).astype(BF16)


def sum_kernel(mine, peer, *refs):
    refs[-1][...] = (mine[...].astype(F32) + peer[...].astype(F32)).astype(BF16)


def swap(x, axis, bit):
    size = lax.axis_size(axis)
    return lax.ppermute(x, axis, [(i, i ^ bit) for i in range(size)])


def hop(x, steps):
    size = lax.axis_size("seq")
    pairs = []
    for i in range(size):
        j = (i + 8 * steps if i % 2 == 1 else i - 8 * steps) ^ (4 * (steps % 2))
        if 0 <= j < size:
            pairs.append((i, j))
    return lax.ppermute(x, "seq", pairs)


def call(kernel, outs, *ins, scratch=()):
    return pl.pallas_call(
        kernel,
        in_specs=[VM] * len(ins),
        out_specs=[VM] * len(outs),
        out_shape=[pltpu.VMEM(*o) for o in outs],
        scratch_shapes=list(scratch),
        compiler_params=params(False),
    )(*[vmem(x) for x in ins])


def body(
    inner_acts,
    gate_input,
    forward_keys,
    forward_queries,
    backward_keys,
    backward_queries,
    decay_codes,
    clip_start,
    skip_gain,
    norm_gain,
    out_weight,
):
    tokens, channels = inner_acts.shape
    heads = skip_gain.shape[0]
    spans = decay_codes.shape[1]
    span = tokens // spans
    nstate = forward_keys.shape[1]
    model = out_weight.shape[1]
    chan = lax.axis_size("chan")
    part = channels // 4
    assert spans == 2

    codes = decay_codes.reshape(2 * spans, heads)
    clip = clip_start.reshape(1, tokens)
    skip = skip_gain.reshape(1, heads)
    gain = norm_gain.reshape(1, channels)

    block = min(512, channels // 2)
    steps = channels // block
    tile = lambda rows: pl.BlockSpec((rows, block), lambda i: (0, i))
    full = lambda x: pl.BlockSpec(x.shape, lambda i: (0, 0))
    vshape = pltpu.VMEM

    send, keep, midf, midb, rows = pl.pallas_call(
        functools.partial(local_kernel, float(lax.axis_size("seq") * tokens), channels // heads),
        grid=(steps,),
        in_specs=[tile(tokens), full(forward_keys), full(backward_keys), full(codes), full(skip), full(clip)],
        out_specs=[VM] * 5,
        out_shape=[
            vshape((nstate + 8, channels), BF16), vshape((nstate, channels), F32), vshape((nstate, channels), BF16),
            vshape((nstate, channels), BF16), vshape((24, channels), F32),
        ],
        scratch_shapes=[pltpu.VMEM((2, tokens, nstate), BF16)],
        compiler_params=params(),
        name="local",
    )(*[hbm(x) for x in (inner_acts, forward_keys, backward_keys, codes, skip, clip)])

    recv1 = swap(send, "seq", 1)
    packed = ((nstate + 8, part), BF16)
    mine, passes, *sends = call(
        chip_kernel, [((nstate, part), F32), ((8, part), F32)] + [packed] * 3, recv1, keep, rows
    )
    recv2 = [swap(x, "seq", 2 * k + 2) for k, x in enumerate(sends)]

    keys = [forward_keys, backward_keys, forward_queries, backward_queries]
    scores, query = call(
        score_kernel, [((2 * spans, span, span), BF16), ((2, tokens, nstate), BF16)], sends[0], *keys, clip
    )
    inner_shapes = [
        vshape((tokens, channels), F32), vshape((tokens, channels), BF16), vshape((tokens, channels), BF16),
        vshape(out_weight.shape, BF16),
    ]

    def inner(first, after, prior):
        off = 0 if first else steps // 2
        wide = pl.BlockSpec((tokens, block), lambda i: (0, i + off))
        return pl.pallas_call(
            functools.partial(inner_kernel, first),
            grid=(max(steps // 2, 1),),
            in_specs=[VM, wide, wide, VM, VM, VM, VM, VM, pl.BlockSpec(memory_space=pltpu.HBM)] + [VM] * len(prior),
            out_specs=[VM] * 4,
            out_shape=inner_shapes,
            input_output_aliases={9 + k: k for k in range(len(prior))},
            scratch_shapes=[pltpu.SemaphoreType.DMA],
            compiler_params=params(),
            cost_estimate=pl.CostEstimate(flops=2 * 10**9, transcendentals=0, bytes_accessed=8 * 2**20),
            name="inner",
        )(
            vmem(after), inner_acts, gate_input, *[vmem(v) for v in (rows, midf, midb, scores, query)], hbm(out_weight),
            *[vmem(v) for v in prior],
        )

    half_done = inner(True, sends[0], [])

    total, states, decays = call(
        group_kernel, [packed, ((4, nstate, part), F32), ((4, 8, part), F32)], *recv2, mine, passes, scores
    )
    yg, gf, gb, weight = inner(False, total, half_done)
    blocks = lax.axis_size("seq") // 8
    if blocks == 2:
        before = swap(total, "seq", 12)
    else:
        step = 1
        while step < blocks:
            (total,) = call(join_kernel, [packed], total, hop(total, step))
            step *= 2
        before = hop(total, 1)
    own = call(
        functools.partial(entry_kernel, blocks == 2), [((nstate, part), BF16)] * 4, before, states, decays, weight,
        scratch=[pltpu.VMEM((4, nstate, part), F32)],
    )
    arrived = [own[0]]
    for k, x in enumerate(own[1:]):
        arrived.append(swap(x, "seq", 2 * k + 2))
    own = arrived
    peer = []
    for x in own:
        peer.append(swap(x, "seq", 1))

    def carry(pieces, span_at, last, before):
        length = span_at[1] - span_at[0]
        sums = ((8, length), F32) if last else ((length, 128), F32)
        return call(
            functools.partial(carry_kernel, pieces, span_at, last), [((length, part), BF16)] * len(pieces) + [sums],
            *[own[k] for k in pieces], *[peer[k] for k in pieces], yg, gf, gb, recv1, query, gain, *before,
        )

    done_0, acc = carry((0,), (0, tokens), False, [])
    done_1, acc = carry((1,), (0, tokens), False, [acc])
    done_2, acc = carry((2,), (0, tokens), False, [acc])
    done_3, squares = carry((3,), (0, tokens), True, [acc])
    if chan == 2:
        others = swap(squares, "chan", 1)
    else:
        squares, others = lax.psum(squares, "chan"), jnp.zeros_like(squares)
    out_rows = tokens // POOL
    first = model // 4
    done = [done_0, done_1, done_2, done_3]
    tokens_high, tokens_low = call(early_kernel, [((tokens, first), BF16)] * 2, *done, weight)
    mixed, high, low = call(
        functools.partial(first_kernel, float(channels * chan)),
        [((out_rows, first), BF16), ((out_rows, tokens), BF16), ((out_rows, tokens), BF16)],
        squares, others, tokens_high, tokens_low,
    )
    (pooled,) = call(pool_kernel, [((out_rows, channels), BF16)], *done, high, low)
    chunks = [(0, first), (first, model - first), (model - first, model)]
    out = None
    for k, (start, stop) in enumerate(chunks):
        if k:
            (mixed,) = call(
                functools.partial(project_kernel, start), [((out_rows, stop - start), BF16)], pooled, weight
            )
        if chan == 2:
            others = swap(mixed, "chan", 1)
        else:
            mixed, others = lax.psum(mixed.astype(F32), "chan").astype(BF16), jnp.zeros_like(mixed)
        prior = [] if out is None else [out]
        share = pl.BlockSpec((out_rows, first), lambda i: (0, i))
        out = pl.pallas_call(
            sum_kernel,
            grid=(mixed.shape[1] // first,),
            in_specs=[share, share] + [pl.BlockSpec(memory_space=pl.ANY)] * len(prior),
            out_specs=pl.BlockSpec((out_rows, first), lambda i, at=start // first: (0, i + at)),
            out_shape=jax.ShapeDtypeStruct((out_rows, model), BF16),
            input_output_aliases={2: 0} if prior else {},
            compiler_params=params(),
            name="sum",
        )(vmem(mixed), vmem(others), *prior)
    return out


def solution(mesh):
    placed = (
        P("seq", "chan"),
        P("seq", "chan"),
        P("seq", None),
        P("seq", None),
        P("seq", None),
        P("seq", None),
        P(None, "seq", "chan"),
        P("seq"),
        P("chan"),
        P("chan"),
        P("chan", None),
    )
    return jax.shard_map(body, mesh=mesh, in_specs=placed, out_specs=P("seq", None), check_vma=False)
```

```python
import functools
import math

import jax
import jax.numpy as jnp
from jax import lax
from jax.experimental import pallas as pl
from jax.experimental.pallas import tpu as pltpu
from jax.sharding import PartitionSpec as P


POOL = 4
EPS = 1e-05
LOG2E = math.log2(math.e)
F32 = jnp.float32
BF16 = jnp.bfloat16


VM = pl.BlockSpec(memory_space=pltpu.VMEM)


def params(grid=True, mib=16):
    kw = {"dimension_semantics": ("arbitrary",)} if grid else {}
    return pltpu.CompilerParams(vmem_limit_bytes=mib * 1024 * 1024, **kw)


def vmem(x):
    return pltpu.with_memory_space_constraint(x, pltpu.VMEM)


def hbm(x):
    return pltpu.with_memory_space_constraint(x, pltpu.HBM)


def dot(a, b, dims=((1,), (0,)), precision=None):
    return lax.dot_general(a, b, (dims, ((), ())), precision=precision, preferred_element_type=F32)


def place():
    index = lax.axis_index("seq")
    block = index // 8
    return index % 2 == 1, (index // 2) % 4, block, 2 * (block % 2)


def lanes(start, count):
    return pl.ds(pl.multiple_of(start, 128), count)


def split_rows(v):
    high = v.astype(BF16)
    low = (v - high.astype(F32)).astype(BF16)
    return jnp.concatenate([high, low, jnp.zeros((6, v.shape[1]), BF16)], axis=0)


def joined(ref, nstate, at=slice(None)):
    rows = ref[nstate : nstate + 8, at].astype(F32)
    return rows[0:1] + rows[1:2]


def token_masks(row):
    span = row.shape[1]
    rows = lax.broadcasted_iota(jnp.int32, (span, span), 0)
    cols = lax.broadcasted_iota(jnp.int32, (span, span), 1)
    seg = jnp.sum(jnp.where(cols <= rows, row, 0.0), axis=1, keepdims=True)
    count = jnp.sum(row, axis=1, keepdims=True)
    return seg, count, rows, cols


def local_kernel(total, size, block, *refs):
    sources, refs = refs[:9], refs[9:]
    send, keep, midf, midb, rows, x, gate, qf, qb, kf, kb, clip, skip, codes, keys, sems = refs
    targets = (clip, kf, kb, codes, skip, x, gate, qf, qb)
    spans = 2
    span = clip.shape[1] // spans
    channels = x.shape[1]
    nstate = kf.shape[1]
    steps = channels // block
    own_f, _, _, _ = place()
    copies = []
    for source, target in zip(sources, targets):
        parts = [slice(None)]
        if target is x:
            parts = [pl.ds(i * block, block) for i in range(steps)]
        for part in parts:
            copies.append(pltpu.make_async_copy(source.at[:, part], target.at[:, part], sems.at[len(copies)]))
            copies[-1].start()
    for k in range(5):
        copies[k].wait()

    wholes = []
    for s in range(spans):
        at = slice(s * span, (s + 1) * span)
        seg, count, _, _ = token_masks(clip[0:1, at].astype(F32))
        keys[0, at, :] = jnp.where(seg == count, kf[at, :].astype(F32), 0.0).astype(BF16)
        keys[1, at, :] = jnp.where(seg == 0.0, kb[at, :].astype(F32), 0.0).astype(BF16)
        wholes.append(count == 0.0)

    heads = codes.shape[1]
    table = jnp.concatenate([codes[...].astype(F32), skip[...], jnp.zeros((3, heads), F32)], axis=0)
    lane = lax.broadcasted_iota(jnp.int32, (heads, channels), 1)
    pick = lax.broadcasted_iota(jnp.int32, (heads, channels), 0) == lane // size
    wide = dot(table, jnp.where(pick, 1.0, 0.0), precision=lax.Precision.HIGHEST)
    rate_all = wide[0:4] * (1.0 / (32.0 * total))
    log_all = jnp.log1p(-rate_all) * LOG2E
    scal_all = jnp.sqrt(rate_all * (2.0 - rate_all))
    rows[8:16, :] = jnp.concatenate([log_all, scal_all], axis=0)
    rows[16:24, :] = jnp.concatenate([wide[4:5], wide[1:8]], axis=0)

    group = 16
    count = span // group
    near = lax.broadcasted_iota(jnp.int32, (group, 1), 0).astype(F32)
    far = lax.broadcasted_iota(jnp.int32, (count, 1), 0).astype(F32) * group
    for i in range(steps):
        here = slice(i * block, (i + 1) * block)
        logd, scal = log_all[:, here], scal_all[:, here]
        copies[5 + i].wait()
        lf, lb, pf, pb, df, db = [], [], [], [], [], []
        for s in range(spans):
            log_f, log_b = logd[s : s + 1], logd[2 + s : 3 + s]
            near_f = scal[s : s + 1] * jnp.exp2((group - 1.0 - near) * log_f)
            near_b = scal[2 + s : 3 + s] * jnp.exp2(near * log_b)
            far_f = jnp.exp2((span - group - far) * log_f)
            far_b = jnp.exp2(far * log_b)
            xs_f, xs_b = [], []
            for a in range(count):
                acts = x[s * span + a * group : s * span + (a + 1) * group, here].astype(F32)
                xs_f.append((acts * near_f * far_f[a : a + 1]).astype(BF16))
                xs_b.append((acts * near_b * far_b[a : a + 1]).astype(BF16))
            at = slice(s * span, (s + 1) * span)
            lf.append(dot(keys[0, at, :], jnp.concatenate(xs_f, axis=0), ((0,), (0,))))
            lb.append(dot(keys[1, at, :], jnp.concatenate(xs_b, axis=0), ((0,), (0,))))
            d_f, d_b = jnp.exp2(span * log_f), jnp.exp2(span * log_b)
            df.append(d_f)
            db.append(d_b)
            pf.append(jnp.where(wholes[s], d_f, 0.0))
            pb.append(jnp.where(wholes[s], d_b, 0.0))
        loc_f = pf[1] * lf[0] + lf[1]
        loc_b = lb[0] + pb[0] * lb[1]
        all_f, all_b = pf[0] * pf[1], pb[0] * pb[1]
        send[0:nstate, here] = jnp.where(own_f, loc_b, loc_f).astype(BF16)
        send[nstate : nstate + 8, here] = split_rows(jnp.where(own_f, all_b, all_f))
        keep[:, here] = jnp.where(own_f, loc_f, loc_b)
        midf[:, here] = lf[0].astype(BF16)
        midb[:, here] = lb[1].astype(BF16)
        own = jnp.where(own_f, all_f, all_b)
        rows[0:8, here] = jnp.concatenate([own, own, pf[0], pb[1], df[0], df[1], db[0], db[1]], axis=0)
    for copy in copies[5 + steps :]:
        copy.wait()


def score_kernel(after, kf, kb, qf, qb, clip, scores, query):
    spans = 2
    span = clip.shape[1] // spans
    for s in range(spans):
        at = slice(s * span, (s + 1) * span)
        row = clip[0:1, at].astype(F32)
        seg, count, rows, cols = token_masks(row)
        upto = jnp.where(rows <= cols, 1.0, 0.0).astype(BF16)
        seg_row = dot(jnp.broadcast_to(row, (8, span)).astype(BF16), upto)[0:1, :]
        same = seg == seg_row
        sf = dot(qf[at, :], kf[at, :], ((1,), (1,)))
        sb = dot(qb[at, :], kb[at, :], ((1,), (1,)))
        scores[2 * s] = jnp.where(same & (cols <= rows), sf, 0.0).astype(BF16)
        scores[2 * s + 1] = jnp.where(same & (cols >= rows), sb, 0.0).astype(BF16)
        query[0, at, :] = jnp.where(seg == 0.0, qf[at, :].astype(F32), 0.0).astype(BF16)
        query[1, at, :] = jnp.where(seg == count, qb[at, :].astype(F32), 0.0).astype(BF16)


def inner_kernel(first, block, *refs):
    after, x, gate, rows, midf, midb, scores, query, weight, *refs = refs
    if first:
        yg, gf, gb, weight_out, sem = refs
    else:
        yg, gf, gb, weight_out, sem = refs[4:]
    span = scores.shape[1]
    half = x.shape[1] // 2
    height = weight.shape[0] // 2
    band = pl.ds(0 if first else height, height)
    fetch = pltpu.make_async_copy(weight.at[band], weight_out.at[band], sem)

    fetch.start()
    for i in range(half // block):
        base = i * block + (0 if first else half)
        inner_block(slice(base, base + block), span, x, gate, rows, midf, midb, scores, query, yg, gf, gb)
    fetch.wait()


def inner_block(here, span, x, gate, rows, midf, midb, scores, query, yg, gf, gb):
    p = rows[0:8, here]
    logd, scal = rows[8:12, here], rows[12:16, here]
    skip = rows[16:24, here][0:1]
    pos = lax.broadcasted_iota(jnp.int32, (span, 1), 0).astype(F32)
    for s in range(2):
        at = slice(s * span, (s + 1) * span)
        log_f, log_b = logd[s : s + 1], logd[2 + s : 3 + s]
        d_f, d_b = p[4 + s : 5 + s], p[6 + s : 7 + s]
        acts = x[at, here].astype(F32)
        xs_f = (acts * (scal[s : s + 1] * jnp.exp2((span - 1.0 - pos) * log_f))).astype(BF16)
        xs_b = (acts * (scal[2 + s : 3 + s] * jnp.exp2(pos * log_b))).astype(BF16)
        z = gate[at, here].astype(F32)
        g = z / (1.0 + jnp.exp(-z))
        g_f = g * jnp.exp2((pos - (span - 1.0)) * log_f)
        g_b = g * jnp.exp2(-pos * log_b)
        y_f, y_b = dot(scores[2 * s], xs_f), dot(scores[2 * s + 1], xs_b)
        if s == 1:
            y_f = y_f + dot(query[0, at, :], (d_f * midf[:, here].astype(F32)).astype(BF16))
            d_f = d_f * p[2:3]
        else:
            y_b = y_b + dot(query[1, at, :], (d_b * midb[:, here].astype(F32)).astype(BF16))
            d_b = d_b * p[3:4]
        yg[at, here] = g_f * y_f + g_b * y_b + g * (skip * acts)
        gf[at, here] = (g_f * d_f).astype(BF16)
        gb[at, here] = (g_b * d_b).astype(BF16)


def chip_kernel(recv, keep, rows, mine, passes, *sends):
    nstate, part = mine.shape
    _, chip, _, flip = place()
    for k in range(4):
        at = lanes((chip ^ k ^ flip) * part, part)
        own = rows[0:8, at][0:1]
        state = own * recv[0:nstate, at].astype(F32) + keep[:, at]
        both = own * joined(recv, nstate, at)
        if k == 0:
            mine[...] = state
            passes[...] = jnp.broadcast_to(both, (8, part))
        else:
            sends[k - 1][0:nstate, :] = state.astype(BF16)
            sends[k - 1][nstate : nstate + 8, :] = split_rows(both)


def group_kernel(recv_a, recv_b, recv_c, mine, passes, _, total, states, decays):
    nstate = mine.shape[0]
    own_f, chip, _, _ = place()
    states[chip] = mine[...]
    decays[chip] = passes[...]
    for k, recv in enumerate((recv_a, recv_b, recv_c)):
        states[chip ^ (k + 1)] = recv[0:nstate, :].astype(F32)
        decays[chip ^ (k + 1)] = jnp.broadcast_to(joined(recv, nstate), passes.shape)
    first = jnp.where(own_f, 0, 3)
    state, keep = states[first], decays[first][0:1]
    for t in range(1, 4):
        j = jnp.where(own_f, t, 3 - t)
        d = decays[j][0:1]
        state = d * state + states[j]
        keep = keep * d
    total[0:nstate, :] = state.astype(BF16)
    total[nstate : nstate + 8, :] = split_rows(keep)


def join_kernel(mine, recv, total):
    nstate = mine.shape[0] - 8
    keep = joined(mine, nstate)
    total[0:nstate, :] = (mine[0:nstate, :].astype(F32) + keep * recv[0:nstate, :].astype(F32)).astype(BF16)
    total[nstate : nstate + 8, :] = split_rows(keep * joined(recv, nstate))


def entry_kernel(pair, recv, states, decays, _, entry, send_a, send_b, send_c, ahead):
    nstate = entry.shape[0]
    own_f, chip, block, _ = place()
    state = recv[0:nstate, :].astype(F32)
    if pair:
        state = jnp.where(own_f == (block == 1), state, 0.0)
    for t in range(4):
        j = jnp.where(own_f, t, 3 - t)
        ahead[j] = state
        if t < 3:
            state = decays[j][0:1] * state + states[j]
    for k, out in enumerate((entry, send_a, send_b, send_c)):
        out[...] = ahead[chip ^ k].astype(BF16)


def carry_kernel(pieces, tokens, last, *refs):
    count = len(pieces)
    own_refs, oth_refs, refs = refs[:count], refs[count : 2 * count], refs[2 * count :]
    yg, gf, gb, recv, query, gain, *refs = refs
    before = None if pieces[0] == 0 else refs.pop(0)
    gated, sums = refs[:count], refs[count]
    own_f, chip, _, flip = place()
    nstate, part = own_refs[0].shape
    at = slice(*tokens)
    rel = slice(0, tokens[1] - tokens[0])
    acc = jnp.zeros((tokens[1] - tokens[0], 128), F32) if before is None else before[at, :]
    for own_ref, oth_ref, out, piece in zip(own_refs, oth_refs, gated, pieces):
        here = lanes((chip ^ piece ^ flip) * part, part)
        own = joined(recv, nstate, here) * own_ref[...].astype(F32) + recv[0:nstate, here].astype(F32)
        oth = oth_ref[...].astype(F32)
        st_f, st_b = jnp.where(own_f, own, oth).astype(BF16), jnp.where(own_f, oth, own).astype(BF16)
        c_f = dot(query[0, at, :], st_f)
        c_b = dot(query[1, at, :], st_b)
        v = yg[at, here] + gf[at, here].astype(F32) * c_f + gb[at, here].astype(F32) * c_b
        out[rel, :] = (v * gain[0:1, here]).astype(BF16)
        sq = v * v
        for k in range(part // 128):
            acc = acc + sq[:, k * 128 : (k + 1) * 128]
    if last:
        ones = jnp.ones((8, 128), BF16)
        high = acc.astype(BF16)
        low = (acc - high.astype(F32)).astype(BF16)
        sums[...] = dot(ones, high, ((1,), (1,))) + dot(ones, low, ((1,), (1,)))
    else:
        sums[...] = acc


def early_kernel(pieces_a, pieces_b, pieces_c, pieces_d, weight, high, low):
    part = pieces_a.shape[1]
    _, chip, _, flip = place()
    total = None
    for k, ref in enumerate((pieces_a, pieces_b, pieces_c, pieces_d)):
        at = lanes((chip ^ k ^ flip) * part, part)
        term = dot(ref[...], weight[at, 0 : high.shape[1]])
        total = term if total is None else total + term
    high[...] = total.astype(BF16)
    low[...] = (total - high[...].astype(F32)).astype(BF16)


def first_kernel(width, own, other, tokens_high, tokens_low, out, pool_high, pool_low):
    rows, tokens = pool_high.shape
    inv = lax.rsqrt((own[0:1, :] + other[0:1, :]) / width + EPS) * (1.0 / POOL)
    group = lax.broadcasted_iota(jnp.int32, (rows, tokens), 0)
    token = lax.broadcasted_iota(jnp.int32, (rows, tokens), 1)
    pool = jnp.where(token // POOL == group, inv, 0.0)
    high = pool.astype(BF16)
    low = (pool - high.astype(F32)).astype(BF16)
    pool_high[...] = high
    pool_low[...] = low
    out[...] = (dot(high, tokens_high[...]) + dot(high, tokens_low[...]) + dot(low, tokens_high[...])).astype(BF16)


def pool_kernel(pieces_a, pieces_b, pieces_c, pieces_d, high, low, pooled):
    part = pieces_a.shape[1]
    _, chip, _, flip = place()
    for k, ref in enumerate((pieces_a, pieces_b, pieces_c, pieces_d)):
        at = lanes((chip ^ k ^ flip) * part, part)
        pooled[:, at] = (dot(high[...], ref[...]) + dot(low[...], ref[...])).astype(BF16)


def project_kernel(start, pooled, weight, out):
    out[...] = dot(pooled[...], weight[:, start : start + out.shape[1]]).astype(BF16)


def sum_kernel(mine, peer, *refs):
    refs[-1][...] = (mine[...].astype(F32) + peer[...].astype(F32)).astype(BF16)


def swap(x, axis, bit):
    size = lax.axis_size(axis)
    return lax.ppermute(x, axis, [(i, i ^ bit) for i in range(size)])


def hop(x, steps):
    size = lax.axis_size("seq")
    pairs = []
    for i in range(size):
        j = (i + 8 * steps if i % 2 == 1 else i - 8 * steps) ^ (4 * (steps % 2))
        if 0 <= j < size:
            pairs.append((i, j))
    return lax.ppermute(x, "seq", pairs)


def call(kernel, outs, *ins, scratch=()):
    return pl.pallas_call(
        kernel,
        in_specs=[VM] * len(ins),
        out_specs=[VM] * len(outs),
        out_shape=[pltpu.VMEM(*o) for o in outs],
        scratch_shapes=list(scratch),
        compiler_params=params(False),
    )(*[vmem(x) for x in ins])


def body(
    inner_acts,
    gate_input,
    forward_keys,
    forward_queries,
    backward_keys,
    backward_queries,
    decay_codes,
    clip_start,
    skip_gain,
    norm_gain,
    out_weight,
):
    tokens, channels = inner_acts.shape
    heads = skip_gain.shape[0]
    spans = decay_codes.shape[1]
    span = tokens // spans
    nstate = forward_keys.shape[1]
    model = out_weight.shape[1]
    chan = lax.axis_size("chan")
    part = channels // 4
    assert spans == 2

    codes = decay_codes.reshape(2 * spans, heads)
    clip = clip_start.reshape(1, tokens)
    skip = skip_gain.reshape(1, heads)
    gain = norm_gain.reshape(1, channels)

    block = min(512, channels // 2)
    steps = channels // block
    vshape = pltpu.VMEM

    sources = (clip, forward_keys, backward_keys, codes, skip, inner_acts, gate_input, forward_queries, backward_queries)
    small = (tokens, nstate)
    send, keep, midf, midb, rows, acts, gate, q_f, q_b, k_f, k_b, starts = pl.pallas_call(
        functools.partial(local_kernel, float(lax.axis_size("seq") * tokens), channels // heads, block),
        in_specs=[pl.BlockSpec(memory_space=pltpu.HBM)] * len(sources),
        out_specs=[VM] * 12,
        out_shape=[
            vshape((nstate + 8, channels), BF16), vshape((nstate, channels), F32), vshape((nstate, channels), BF16),
            vshape((nstate, channels), BF16), vshape((24, channels), F32), vshape((tokens, channels), BF16),
            vshape((tokens, channels), BF16), vshape(small, BF16), vshape(small, BF16), vshape(small, BF16),
            vshape(small, BF16), vshape((1, tokens), clip.dtype),
        ],
        scratch_shapes=[
            pltpu.VMEM(skip.shape, skip.dtype), pltpu.VMEM(codes.shape, codes.dtype), pltpu.VMEM((2, tokens, nstate), BF16),
            pltpu.SemaphoreType.DMA((len(sources) - 1 + steps,)),
        ],
        compiler_params=params(False),
        name="local",
    )(*[hbm(v) for v in sources])

    recv1 = swap(send, "seq", 1)
    packed = ((nstate + 8, part), BF16)
    mine, passes, *sends = call(
        chip_kernel, [((nstate, part), F32), ((8, part), F32)] + [packed] * 3, recv1, keep, rows
    )
    recv2 = [swap(x, "seq", 2 * k + 2) for k, x in enumerate(sends)]

    keys = [k_f, k_b, q_f, q_b]
    scores, query = call(
        score_kernel, [((2 * spans, span, span), BF16), ((2, tokens, nstate), BF16)], sends[0], *keys, starts
    )
    inner_shapes = [
        vshape((tokens, channels), F32), vshape((tokens, channels), BF16), vshape((tokens, channels), BF16),
        vshape(out_weight.shape, BF16),
    ]

    def inner(first, after, prior):
        return pl.pallas_call(
            functools.partial(inner_kernel, first, block),
            in_specs=[VM] * 8 + [pl.BlockSpec(memory_space=pltpu.HBM)] + [VM] * len(prior),
            out_specs=[VM] * 4,
            out_shape=inner_shapes,
            input_output_aliases={9 + k: k for k in range(len(prior))},
            scratch_shapes=[pltpu.SemaphoreType.DMA],
            compiler_params=params(False),
            cost_estimate=pl.CostEstimate(flops=2 * 10**9, transcendentals=0, bytes_accessed=8 * 2**20),
            name="inner",
        )(
            vmem(after), *[vmem(v) for v in (acts, gate, rows, midf, midb, scores, query)], hbm(out_weight),
            *[vmem(v) for v in prior],
        )

    half_done = inner(True, sends[0], [])

    total, states, decays = call(
        group_kernel, [packed, ((4, nstate, part), F32), ((4, 8, part), F32)], *recv2, mine, passes, scores
    )
    yg, gf, gb, weight = inner(False, total, half_done)
    blocks = lax.axis_size("seq") // 8
    if blocks == 2:
        before = swap(total, "seq", 12)
    else:
        step = 1
        while step < blocks:
            (total,) = call(join_kernel, [packed], total, hop(total, step))
            step *= 2
        before = hop(total, 1)
    own = call(
        functools.partial(entry_kernel, blocks == 2), [((nstate, part), BF16)] * 4, before, states, decays, weight,
        scratch=[pltpu.VMEM((4, nstate, part), F32)],
    )
    arrived = [own[0]]
    for k, x in enumerate(own[1:]):
        arrived.append(swap(x, "seq", 2 * k + 2))
    own = arrived
    peer = []
    for x in own:
        peer.append(swap(x, "seq", 1))

    def carry(pieces, span_at, last, before):
        length = span_at[1] - span_at[0]
        sums = ((8, length), F32) if last else ((length, 128), F32)
        return call(
            functools.partial(carry_kernel, pieces, span_at, last), [((length, part), BF16)] * len(pieces) + [sums],
            *[own[k] for k in pieces], *[peer[k] for k in pieces], yg, gf, gb, recv1, query, gain, *before,
        )

    done_0, acc = carry((0,), (0, tokens), False, [])
    done_1, acc = carry((1,), (0, tokens), False, [acc])
    done_2, acc = carry((2,), (0, tokens), False, [acc])
    done_3, squares = carry((3,), (0, tokens), True, [acc])
    if chan == 2:
        others = swap(squares, "chan", 1)
    else:
        squares, others = lax.psum(squares, "chan"), jnp.zeros_like(squares)
    out_rows = tokens // POOL
    first = model // 4
    done = [done_0, done_1, done_2, done_3]
    tokens_high, tokens_low = call(early_kernel, [((tokens, first), BF16)] * 2, *done, weight)
    mixed, high, low = call(
        functools.partial(first_kernel, float(channels * chan)),
        [((out_rows, first), BF16), ((out_rows, tokens), BF16), ((out_rows, tokens), BF16)],
        squares, others, tokens_high, tokens_low,
    )
    (pooled,) = call(pool_kernel, [((out_rows, channels), BF16)], *done, high, low)
    chunks = [(0, first), (first, model - first), (model - first, model)]
    out = None
    for k, (start, stop) in enumerate(chunks):
        if k:
            (mixed,) = call(
                functools.partial(project_kernel, start), [((out_rows, stop - start), BF16)], pooled, weight
            )
        if chan == 2:
            others = swap(mixed, "chan", 1)
        else:
            mixed, others = lax.psum(mixed.astype(F32), "chan").astype(BF16), jnp.zeros_like(mixed)
        prior = [] if out is None else [out]
        share = pl.BlockSpec((out_rows, first), lambda i: (0, i))
        out = pl.pallas_call(
            sum_kernel,
            grid=(mixed.shape[1] // first,),
            in_specs=[share, share] + [pl.BlockSpec(memory_space=pl.ANY)] * len(prior),
            out_specs=pl.BlockSpec((out_rows, first), lambda i, at=start // first: (0, i + at)),
            out_shape=jax.ShapeDtypeStruct((out_rows, model), BF16),
            input_output_aliases={2: 0} if prior else {},
            compiler_params=params(),
            name="sum",
        )(vmem(mixed), vmem(others), *prior)
    return out


def solution(mesh):
    placed = (
        P("seq", "chan"),
        P("seq", "chan"),
        P("seq", None),
        P("seq", None),
        P("seq", None),
        P("seq", None),
        P(None, "seq", "chan"),
        P("seq"),
        P("chan"),
        P("chan"),
        P("chan", None),
    )
    return jax.shard_map(body, mesh=mesh, in_specs=placed, out_specs=P("seq", None), check_vma=False)
```
